32 devices in a mesh: gz: 8 (over y, x, core), gy: 4 (over z).
Axes of the slice: x: 2, y: 2, z: 4, core: 2. Of those that a mesh axis runs over, the one named last changes fastest.
Arguments:
- source: float32 [128, 256, 256], P(('gz', 'gy')), may hold values from -8 to 8
- vertical: float32 [128], P(('gz', 'gy')), may hold values from 1 to 64
- reaction: float32 [128, 256, 256], P(('gz', 'gy')), may hold values from 0.05 to 2
Outputs:
- solution: float32 [128, 256, 256], P(('gz', 'gy'))
- norms: float32 [2], replicated
The draws below stay inside these ranges and needn't reach their ends.
All inputs are finite; a program needn't handle non-finite values.
Results may differ from the reference program's by a relative error of at most 0.0001.
Values sent between devices are 32-bit elements; how exact they have to be, the bound alone decides.
A program may use at most 192 MiB of HBM per device.

```python
import math
import jax
import jax.numpy as jnp

NX = 256
LEVELS = 5
SWITCH = 2
CYCLES = 2
SWEEPS = 2
COARSE = 4
NZ = 128


def draw_source(key, part):
    rough = jax.random.truncated_normal(key, -6.0, 6.0, (NZ, NX, NX), jnp.float32)
    return rough


def levels(key, dims, pieces, least, high):
    def one(position, parts):
        steps = jax.random.uniform(jax.random.fold_in(jax.random.fold_in(key, 6), position), (parts,), jnp.float32, least / len(pieces), high / len(pieces))
        return jnp.repeat(jnp.exp(steps), dims[position] // parts).reshape((-1,) + (1,) * (len(dims) - position - 1))

    level = one(*pieces[0])
    for cut in pieces[1:]:
        level = level * one(*cut)
    return level


def setup_inputs(seed: int = 0) -> dict:
    splits = jax.random.split(jax.random.key(seed), 4)
    return {
        "source": draw_source(jax.random.fold_in(splits[3], 71), 0),
        "vertical": jnp.clip(jnp.exp(math.log(64.0) - 4.158883 * jax.random.uniform(splits[1], (NZ,), jnp.float32) ** levels(splits[1], (NZ,), ((0, 32),), -0.2, 0.2)), 1.0, 64.0),
        "reaction": jnp.clip(jnp.exp(math.log(2.0) - 3.6888794 * jax.random.uniform(splits[2], (NZ, NX, NX), jnp.float32) ** levels(splits[2], (NZ, NX, NX), ((0, 32),), -0.2, 0.2)), 0.05, 2.0),
    }


DAMPING = 0.8
COUPLING = 1.0


def plane_sum(values):
    padded = jnp.pad(values, ((0, 0), (1, 1), (1, 1)))
    return padded[:, 2:, 1:-1] + padded[:, :-2, 1:-1] + padded[:, 1:-1, 2:] + padded[:, 1:-1, :-2]


def plane_residual(target, padded, vertical, diagonal, weight):
    centre = padded[1:-1]
    applied = diagonal * centre - vertical * (padded[2:] + padded[:-2]) - weight * plane_sum(centre)
    return target - applied


def around_sum(padded):
    return padded[2:, 1:-1] + padded[:-2, 1:-1] + padded[1:-1, 2:] + padded[1:-1, :-2]


def line_sum(values):
    return around_sum(jnp.pad(values, ((1, 1), (1, 1), (0, 0))))


def shift_left(values, filler):
    return jnp.concatenate([values[..., 1:], jnp.full_like(values[..., :1], filler)], axis=-1)


def shift_right(values, filler):
    return jnp.concatenate([jnp.full_like(values[..., :1], filler), values[..., :-1]], axis=-1)


def odd_even(lower, middle, upper, right):
    length = middle.shape[-1]
    if length == 1:
        return right / middle
    if length % 2 == 1:
        widths = [(0, 0)] * (middle.ndim - 1) + [(0, 1)]
        solved = odd_even(jnp.pad(lower, widths), jnp.pad(middle, widths, constant_values=1.0),
                          jnp.pad(upper, widths), jnp.pad(right, widths))
        return solved[..., :length]
    even_lower = lower[..., 0::2]
    even_middle = middle[..., 0::2]
    even_upper = upper[..., 0::2]
    even_right = right[..., 0::2]
    odd_lower = lower[..., 1::2]
    odd_middle = middle[..., 1::2]
    odd_upper = upper[..., 1::2]
    odd_right = right[..., 1::2]
    next_lower = shift_left(even_lower, 0.0)
    next_middle = shift_left(even_middle, 1.0)
    next_upper = shift_left(even_upper, 0.0)
    next_right = shift_left(even_right, 0.0)
    factor_left = -odd_lower / even_middle
    factor_right = -odd_upper / next_middle
    reduced = odd_even(factor_left * even_lower,
                       odd_middle + factor_left * even_upper + factor_right * next_lower,
                       factor_right * next_upper,
                       odd_right + factor_left * even_right + factor_right * next_right)
    before = shift_right(reduced, 0.0)
    evens = (even_right - even_lower * before - even_upper * reduced) / even_middle
    return jnp.stack([evens, reduced], axis=-1).reshape(middle.shape)


def line_relax(target, around, vertical, diagonal, weight):
    right = target + weight * around
    coupled = jnp.broadcast_to(-vertical, diagonal.shape)
    edge = jnp.zeros_like(coupled[..., :1])
    lower = jnp.concatenate([edge, coupled[..., 1:]], axis=-1)
    upper = jnp.concatenate([coupled[..., :-1], edge], axis=-1)
    return odd_even(lower, diagonal, upper, right)


def line_residual(target, values, around, vertical, diagonal, weight):
    padded = jnp.pad(values, ((0, 0), (0, 0), (1, 1)))
    applied = diagonal * values - vertical * (padded[..., 2:] + padded[..., :-2]) - weight * around
    return target - applied


def shrink_planes(values):
    depth, row_count, column_count = values.shape
    return values.reshape(depth, row_count // 2, 2, column_count // 2, 2).sum(axis=(2, 4)) * 0.25


def grow_planes(values):
    depth, row_count, column_count = values.shape
    spread = jnp.broadcast_to(values[:, :, None, :, None], (depth, row_count, 2, column_count, 2))
    return spread.reshape(depth, 2 * row_count, 2 * column_count)


def shrink_lines(values):
    row_count, column_count, depth = values.shape
    return values.reshape(row_count // 2, 2, column_count // 2, 2, depth).sum(axis=(1, 3)) * 0.25


def grow_lines(values):
    row_count, column_count, depth = values.shape
    spread = jnp.broadcast_to(values[:, None, :, None, :], (row_count, 2, column_count, 2, depth))
    return spread.reshape(2 * row_count, 2 * column_count, depth)


def pad_planes(values):
    return jnp.pad(values, ((1, 1), (0, 0), (0, 0)))


def reference(source, vertical, reaction):
    vertical_col = vertical.reshape(-1, 1, 1)
    reactions = [reaction]
    for height in range(1, LEVELS):
        if height < SWITCH:
            reactions.append(shrink_planes(reactions[-1]))
        elif height == SWITCH:
            reactions.append(jnp.transpose(shrink_planes(reactions[-1]), (1, 2, 0)))
        else:
            reactions.append(shrink_lines(reactions[-1]))
    weights = [COUPLING / 4.0 ** height for height in range(LEVELS)]
    diagonals = []
    for height in range(LEVELS):
        coefficient = vertical_col if height < SWITCH else vertical
        diagonals.append(2.0 * coefficient + 4.0 * weights[height] + reactions[height])

    def descend(height, values, target):
        weight = weights[height]
        diagonal = diagonals[height]
        if height < SWITCH:
            def sweep_plane(values):
                residual = plane_residual(target, pad_planes(values), vertical_col, diagonal, weight)
                return values + DAMPING * residual / diagonal

            for repeat in range(SWEEPS):
                values = sweep_plane(values)
            residual = plane_residual(target, pad_planes(values), vertical_col, diagonal, weight)
            coarse = shrink_planes(residual)
            if height + 1 == SWITCH:
                coarse = jnp.transpose(coarse, (1, 2, 0))
                correction = descend(height + 1, jnp.zeros_like(coarse), coarse)
                correction = jnp.transpose(correction, (2, 0, 1))
            else:
                correction = descend(height + 1, jnp.zeros_like(coarse), coarse)
            values = values + grow_planes(correction)
            for repeat in range(SWEEPS):
                values = sweep_plane(values)
            return values

        def relax_line(values):
            return line_relax(target, line_sum(values), vertical, diagonal, weight)

        if height == LEVELS - 1:
            for repeat in range(COARSE):
                values = relax_line(values)
            return values
        for repeat in range(SWEEPS):
            values = relax_line(values)
        residual = line_residual(target, values, line_sum(values), vertical, diagonal, weight)
        coarse = shrink_lines(residual)
        correction = descend(height + 1, jnp.zeros_like(coarse), coarse)
        values = values + grow_lines(correction)
        for repeat in range(SWEEPS):
            values = relax_line(values)
        return values

    solution = jnp.zeros_like(source)
    scores = []
    for cycle_index in range(CYCLES):
        solution = descend(0, solution, source)
        residual = plane_residual(source, pad_planes(solution), vertical_col, diagonals[0], weights[0])
        scores.append(jnp.mean(residual * residual))
    return solution, jnp.stack(scores)
```

```python
import functools

import jax
import jax.numpy as jnp
import numpy as np
from jax import lax
from jax.experimental import pallas as pl
from jax.experimental.pallas import tpu as pltpu
from jax.sharding import PartitionSpec as P

LEVELS = 5
SWITCH = 2
CYCLES = 2
SWEEPS = 2
COARSE = 4
DAMPING = 0.8
COUPLING = 1.0
CHUNK = 32
MESH = pl.DeviceIdType.MESH


def dot(a, b):
    return lax.dot_general(
        a,
        b,
        (((1,), (0,)), ((), ())),
        precision=lax.Precision.HIGHEST,
        preferred_element_type=jnp.float32,
    )


def kernel(
    dims,
    source, reaction, vert_s, vert_b, down0, downt0, down1, cols, mask, group, ups, groupt, colst,
    out, norms,
    v0, v1, w0, d1, w1, g1, r1, tmp0, res1, corr1, send_a, recv_a, send_v, recv_v, recv_b,
    send_n, recv_n, lines, diag, factor, target, around, halo, rowbuf, acc,
    plane_send, plane_recv, line_send, line_recv, a2a_send, a2a_recv,
):
    gz, gy, depth, cp = dims
    nd = gz * gy
    zall = nd * depth
    n0 = source.shape[1]
    n1 = n0 // 2
    a_me = lax.axis_index("gz")
    b_me = lax.axis_index("gy")
    me = a_me * gy + b_me
    h = [COUPLING / 4.0**k for k in range(LEVELS)]

    @pl.when(me == 0)
    def _():
        for p in range(2):
            v0[p, 0] = jnp.zeros((n0, n0), jnp.float32)
            v1[p, 0] = jnp.zeros((n1, n1), jnp.float32)

    @pl.when(me == nd - 1)
    def _():
        for p in range(2):
            v0[p, depth + 1] = jnp.zeros((n0, n0), jnp.float32)
            v1[p, depth + 1] = jnp.zeros((n1, n1), jnp.float32)

    edges = [a_me == 0, a_me == gz - 1, b_me == 0, b_me == gy - 1]
    for k in range(4):
        @pl.when(edges[k])
        def _(k=k):
            for p in range(2):
                halo[p, k] = jnp.zeros((zall, cp), jnp.float32)

    def flat(d):
        return (d // gy, d % gy)

    def plane_copy(v, p, level, up):
        if up:
            src, dst, to = v.at[p, depth], v.at[p, 0], flat(me + 1)
        else:
            src, dst, to = v.at[p, 1], v.at[p, depth + 1], flat(me + nd - 1 - nd * ((me + nd - 1) // nd))
        if up:
            to = flat((me + 1) % nd)
        k = 0 if up else 1
        return pltpu.make_async_remote_copy(
            src_ref=src, dst_ref=dst,
            send_sem=plane_send.at[level, p, k], recv_sem=plane_recv.at[level, p, k],
            device_id=to, device_id_type=MESH,
        )

    def plane_start(v, p, level):
        @pl.when(me < nd - 1)
        def _():
            plane_copy(v, p, level, True).start()

        @pl.when(me > 0)
        def _():
            plane_copy(v, p, level, False).start()

    def plane_wait(v, p, level):
        @pl.when(me < nd - 1)
        def _():
            plane_copy(v, p, level, True).wait_send()
            plane_copy(v, p, level, False).wait_recv()

        @pl.when(me > 0)
        def _():
            plane_copy(v, p, level, False).wait_send()
            plane_copy(v, p, level, True).wait_recv()

    def residual_chunk(v, p, z, r, n, target_ref, diag_of, weight):
        centre = v[p, z, pl.ds(r, CHUNK), :]
        rows = lax.broadcasted_iota(jnp.int32, (CHUNK, n), 0)
        lanes = lax.broadcasted_iota(jnp.int32, (CHUNK, n), 1)
        if r == 0:
            above = jnp.where(rows == 0, 0.0, pltpu.roll(centre, 1, 0))
        else:
            above = v[p, z, pl.ds(r - 1, CHUNK), :]
        if r + CHUNK == n:
            below = jnp.where(rows == CHUNK - 1, 0.0, pltpu.roll(centre, CHUNK - 1, 0))
        else:
            below = v[p, z, pl.ds(r + 1, CHUNK), :]
        left = jnp.where(lanes == 0, 0.0, pltpu.roll(centre, 1, 1))
        right = jnp.where(lanes == n - 1, 0.0, pltpu.roll(centre, n - 1, 1))
        vert = vert_s[z - 1]
        applied = (
            diag_of(z - 1, r, vert) * centre
            - vert * (v[p, z - 1, pl.ds(r, CHUNK), :] + v[p, z + 1, pl.ds(r, CHUNK), :])
            - weight * (above + below + left + right)
        )
        return centre, target_ref[z - 1, pl.ds(r, CHUNK), :] - applied

    def diag0(z, r, vert):
        return 2.0 * vert + 4.0 * h[0] + reaction[z, pl.ds(r, CHUNK), :]

    def diag1(z, r, vert):
        return d1[z, pl.ds(r, CHUNK), :]

    def over_planes(v, p, level, body):
        plane_start(v, p, level)

        def inner(z, c):
            body(z)
            return c

        lax.fori_loop(2, depth, inner, 0)
        plane_wait(v, p, level)

        def outer(i, c):
            body(1 + i * (depth - 1))
            return c

        lax.fori_loop(0, 2, outer, 0)

    def level_parts(level):
        if level == 0:
            return v0, source, diag0, w0, n0
        return v1, g1, diag1, w1, n1

    def sweep(level, p, record=None):
        v, tgt, dg, w, n = level_parts(level)

        def body(z):
            for r in range(0, n, CHUNK):
                centre, res = residual_chunk(v, p, z, r, n, tgt, dg, h[level])
                v[1 - p, z, pl.ds(r, CHUNK), :] = centre + w[z - 1, pl.ds(r, CHUNK), :] * res
                if record is not None:
                    sq = (res * res).reshape(CHUNK // 8, 8, n).sum(axis=0)
                    acc[record, :, :] += sq

        over_planes(v, p, level, body)
        return 1 - p

    def first_sweep(level):
        v, tgt, dg, w, n = level_parts(level)

        def body(z, c):
            v[0, z + 1] = w[z] * tgt[z]
            return c

        lax.fori_loop(0, depth, body, 0)
        return 0

    def restrict0(read_chunk, store):
        def body(z):
            for r in range(0, n0, CHUNK):
                tmp0[pl.ds(r, CHUNK), :] = dot(read_chunk(z, r), downt0[...])
            store(z, dot(down0[...], tmp0[...]))
        return body

    def restrict1(z, plane):
        half = dot(down1[...], plane)
        for b in range(gy):
            spread = dot(half, cols[b]) * mask[...]
            packed = dot(group[...], spread)
            for a in range(gz):
                send_a[b, a, z : z + 1, :] = packed[a : a + 1, :]

    def exchange_all(kind, src_of, recv):
        def copy(k):
            dst = (me + k) % nd
            a, b = dst // gy, dst % gy
            return pltpu.make_async_remote_copy(
                src_ref=src_of(a, b), dst_ref=recv.at[b_me, a_me],
                send_sem=a2a_send.at[kind, k], recv_sem=a2a_recv.at[kind, me],
                device_id=(a, b), device_id_type=MESH,
            )

        def start(k, c):
            copy(k).start()
            return c

        def finish(k, c):
            copy(k).wait_send()
            src = (me + k) % nd
            a, b = src // gy, src % gy
            pltpu.make_async_remote_copy(
                src_ref=recv.at[b, a], dst_ref=recv.at[b, a],
                send_sem=a2a_send.at[kind, k], recv_sem=a2a_recv.at[kind, src],
                device_id=(a, b), device_id_type=MESH,
            ).wait_recv()
            return c

        def begin():
            lax.fori_loop(1, nd, start, 0)

        def end():
            lax.fori_loop(1, nd, finish, 0)

        return begin, end

    def to_lines(recv, dest):
        for a in range(gz):
            for b in range(gy):
                s = (a * gy + b) * depth
                dest[s : s + depth, :] = recv[b, a]

    bx2, by2 = (n1 // 2 // gz, n1 // 2 // gy)
    steps = []
    s = 1
    while s < zall:
        steps.append(s)
        s *= 2
    ns = len(steps)

    def setup_lines(offset):
        rows = lax.broadcasted_iota(jnp.int32, (zall, cp), 0)
        vert = lines[...]
        a = jnp.where(rows == 0, 0.0, -vert)
        c = jnp.where(rows == zall - 1, 0.0, -vert)
        b = diag[offset]
        for k, s in enumerate(steps):
            alpha = -a / pltpu.roll(b, s, 0)
            gamma = -c / pltpu.roll(b, zall - s, 0)
            b = b + alpha * pltpu.roll(c, s, 0) + gamma * pltpu.roll(a, zall - s, 0)
            a = alpha * pltpu.roll(a, s, 0)
            c = gamma * pltpu.roll(c, zall - s, 0)
            factor[offset, 2 * k] = alpha
            factor[offset, 2 * k + 1] = gamma
        factor[offset, 2 * ns] = 1.0 / b

    def solve(offset, right):
        for k, s in enumerate(steps):
            right = (
                right
                + factor[offset, 2 * k] * pltpu.roll(right, s, 0)
                + factor[offset, 2 * k + 1] * pltpu.roll(right, zall - s, 0)
            )
        return right * factor[offset, 2 * ns]

    count = [0]
    def line_copy(p, k):
        if k == 0:
            to, slot = ((a_me + gz - 1) % gz, b_me), 1
        elif k == 1:
            to, slot = ((a_me + 1) % gz, b_me), 0
        elif k == 2:
            to, slot = (a_me, (b_me + gy - 1) % gy), 3
        else:
            to, slot = (a_me, (b_me + 1) % gy), 2
        return pltpu.make_async_remote_copy(
            src_ref=around.at[p], dst_ref=halo.at[p, slot],
            send_sem=line_send.at[p, k], recv_sem=line_recv.at[p, slot],
            device_id=to, device_id_type=MESH,
        )

    def line_landed(p, k):
        return pltpu.make_async_remote_copy(
            src_ref=around.at[p], dst_ref=halo.at[p, k],
            send_sem=line_send.at[p, k], recv_sem=line_recv.at[p, k],
            device_id=(a_me, b_me), device_id_type=MESH,
        )

    def neighbours(offset, values):
        bx, by = bx2 >> offset, by2 >> offset
        cells = bx * by
        p = count[0] % 2
        count[0] += 1
        around[p] = values
        for k in range(4):
            @pl.when(jnp.logical_not(edges[k]))
            def _(k=k):
                line_copy(p, k).start()
        for k in range(4):
            @pl.when(jnp.logical_not(edges[k]))
            def _(k=k):
                line_copy(p, k).wait_send()
                line_landed(p, k).wait_recv()
        lane = lax.broadcasted_iota(jnp.int32, (zall, cp), 1)

        def roll(x, amount):
            amount = amount % cp
            return x if amount == 0 else pltpu.roll(x, amount, 1)

        total = jnp.where(lane < by, roll(halo[p, 0], by - cells), roll(values, by))
        total += jnp.where(lane >= cells - by, roll(halo[p, 1], cells - by), roll(values, -by))
        inrow = lane & (by - 1)
        total += jnp.where(inrow == 0, roll(halo[p, 2], 1 - by), roll(values, 1))
        total += jnp.where(inrow == by - 1, roll(halo[p, 3], by - 1), roll(values, -1))
        return total

    def line_descend(offset):
        weight = h[SWITCH + offset]
        values = solve(offset, target[offset])
        repeats = COARSE if offset == LEVELS - 1 - SWITCH else SWEEPS
        for _ in range(1, repeats):
            values = solve(offset, target[offset] + weight * neighbours(offset, values))
        if offset == LEVELS - 1 - SWITCH:
            return values
        near = neighbours(offset, values)
        rows = lax.broadcasted_iota(jnp.int32, (zall, cp), 0)
        before = jnp.where(rows == 0, 0.0, pltpu.roll(values, 1, 0))
        after = jnp.where(rows == zall - 1, 0.0, pltpu.roll(values, zall - 1, 0))
        res = target[offset] - (
            diag[offset] * values - lines[...] * (before + after) - weight * near
        )
        target[offset + 1] = dot(res, ups[2 * offset])
        tmp = values
        lower = line_descend(offset + 1)
        values = tmp + dot(lower, ups[2 * offset + 1])
        for _ in range(SWEEPS):
            values = solve(offset, target[offset] + weight * neighbours(offset, values))
        return values

    def fill0(z, c):
        w0[z] = DAMPING / (2.0 * vert_s[z] + 4.0 * h[0] + reaction[z])
        return c

    lax.fori_loop(0, depth, fill0, 0)

    def keep_r1(z, value):
        r1[z] = value
        dv = 2.0 * vert_s[z] + 4.0 * h[1] + value
        d1[z] = dv
        w1[z] = DAMPING / dv

    body = restrict0(lambda z, r: reaction[z, pl.ds(r, CHUNK), :], keep_r1)
    lax.fori_loop(0, depth, lambda z, c: (body(z), c)[1], 0)
    for z in range(depth):
        restrict1(z, r1[z])
    send_v[...] = send_a[...]
    begin_v, end_v = exchange_all(0, lambda a, b: vert_b, recv_v)
    begin_r, end_r = exchange_all(1, lambda a, b: send_v.at[b, a], recv_a)
    begin_v()
    begin_r()
    recv_v[b_me, a_me] = vert_b[...]
    recv_a[b_me, a_me] = send_v[b_me, a_me]
    acc[...] = jnp.zeros_like(acc)

    begin_a, end_a = exchange_all(2, lambda a, b: send_a.at[b, a], recv_b.at[0])
    begin_b, end_b = exchange_all(3, lambda a, b: send_n.at[b, a], recv_b.at[1])

    p0 = first_sweep(0)
    for cycle in range(CYCLES):
        for k in range(SWEEPS):
            if cycle == 0 and k == 0:
                continue
            p0 = sweep(0, p0, record=cycle - 1 if cycle > 0 and k == 0 else None)

        def read0(z, r, p0=p0):
            return residual_chunk(v0, p0, z, r, n0, source, diag0, h[0])[1]

        def keep_g1(z, value):
            g1[z - 1] = value

        over_planes(v0, p0, 0, restrict0(read0, keep_g1))
        p1 = first_sweep(1)
        for k in range(1, SWEEPS):
            p1 = sweep(1, p1)

        def keep_res(z, p1=p1):
            for r in range(0, n1, CHUNK):
                res1[z - 1, pl.ds(r, CHUNK), :] = residual_chunk(
                    v1, p1, z, r, n1, g1, diag1, h[1]
                )[1]

        over_planes(v1, p1, 1, keep_res)
        for z in range(depth):
            restrict1(z, res1[z])
        begin_a()
        recv_b[0, b_me, a_me] = send_a[b_me, a_me]
        if cycle == 0:
            end_v()
            end_r()
            to_lines(recv_v, lines)
            to_lines(recv_a, target.at[0])
            coarse = target[0]
            for offset in range(LEVELS - SWITCH):
                if offset > 0:
                    coarse = dot(coarse, ups[2 * offset - 2])
                diag[offset] = 2.0 * lines[...] + 4.0 * h[SWITCH + offset] + coarse
            for offset in range(LEVELS - SWITCH):
                setup_lines(offset)
        end_a()
        to_lines(recv_b.at[0], target.at[0])
        rowbuf[...] = line_descend(0)
        for a in range(gz):
            for b in range(gy):
                s = (a * gy + b) * depth
                send_n[b, a] = rowbuf[s : s + depth, :]
        begin_b()
        recv_b[1, b_me, a_me] = send_n[b_me, a_me]
        end_b()
        for z in range(depth):
            wide = None
            for b in range(gy):
                for a in range(gz):
                    corr1[a : a + 1, :] = recv_b[1, b, a, z : z + 1, :]
                part = dot(dot(groupt[...], corr1[...]) * mask[...], colst[b])
                wide = part if wide is None else wide + part
            v1[1 - p1, z + 1] = v1[p1, z + 1] + dot(down1[...].T * 2.0, wide)
        p1 = 1 - p1
        for _ in range(SWEEPS):
            p1 = sweep(1, p1)

        def correct0(z, c, p0=p0, p1=p1):
            tmp0[...] = dot(down0[...].T * 2.0, v1[p1, z])
            for r in range(0, n0, CHUNK):
                v0[1 - p0, z, pl.ds(r, CHUNK), :] = v0[p0, z, pl.ds(r, CHUNK), :] + dot(
                    tmp0[pl.ds(r, CHUNK), :], downt0[...].T * 2.0
                )
            return c

        lax.fori_loop(1, depth + 1, correct0, 0)
        p0 = 1 - p0
        for _ in range(SWEEPS):
            p0 = sweep(0, p0)

    def last(z, p0=p0):
        for r in range(0, n0, CHUNK):
            centre, res = residual_chunk(v0, p0, z, r, n0, source, diag0, h[0])
            out[z - 1, pl.ds(r, CHUNK), :] = centre
            acc[CYCLES - 1, :, :] += (res * res).reshape(CHUNK // 8, 8, n0).sum(axis=0)

    over_planes(v0, p0, 0, last)
    ridx = lax.broadcasted_iota(jnp.int32, (8, 128), 0)
    part = jnp.zeros((8, 128), jnp.float32)
    for k in range(CYCLES):
        part = jnp.where(ridx == k, jnp.sum(acc[k]), part)
    rowbuf_n = tmp_n = send_n
    target_n = recv_n
    w_n = acc
    acc[0, :, 0:128] = part
    begin_n, end_n = exchange_all(4, lambda a, b: acc.at[0, :, pl.ds(0, 128)], recv_n)
    begin_n()
    recv_n[b_me, a_me] = part
    end_n()
    total = jnp.zeros((8, 128), jnp.float32)
    for a in range(gz):
        for b in range(gy):
            total = total + recv_n[b, a]
    norms[...] = total * (1.0 / (zall * n0 * n0))


def pair_matrix(n, value):
    return (np.arange(n)[None, :] // 2 == np.arange(n // 2)[:, None]).astype(np.float32) * value


def shards(gz, gy, source, vertical, reaction):
    depth, n0 = source.shape[0], source.shape[1]
    nd = gz * gy
    zall = nd * depth
    n1, n2 = n0 // 2, n0 // 4
    bx, by = n2 // gz, n2 // gy
    cells = bx * by
    cp = -(-cells // 128) * 128
    down0 = pair_matrix(n0, 0.5)
    down1 = pair_matrix(n1, 0.5)
    lane = np.arange(cp)
    cols = np.zeros((gy, n1, cp), np.float32)
    colst = np.zeros((gy, cp, n1), np.float32)
    for b in range(gy):
        hit = (np.arange(n1)[:, None] // 2 == b * by + lane[None, :] % by) & (lane[None, :] < cells)
        cols[b] = hit * 0.5
        colst[b] = hit.T
    mask = ((lane[None, :] // by == np.arange(n2)[:, None] % bx) & (lane[None, :] < cells)).astype(np.float32)
    group = (np.arange(n2)[None, :] // bx == np.arange(gz)[:, None]).astype(np.float32)
    ups = []
    for offset in range(LEVELS - SWITCH - 1):
        fx, fy = bx >> offset, by >> offset
        cy = fy // 2
        matrix = np.zeros((cp, cp), np.float32)
        for i in range(fx):
            for j in range(fy):
                matrix[i * fy + j, (i // 2) * cy + j // 2] = 1.0
        ups += [matrix * 0.25, matrix.T]
    ups = np.stack(ups)
    steps = (zall - 1).bit_length()
    f32 = jnp.float32
    nl = LEVELS - SWITCH
    vm = pl.BlockSpec(memory_space=pltpu.VMEM)
    consts = [down0, down0.T.copy(), down1, cols, mask, group, ups, group.T.copy(), colst]
    solution, norms = pl.pallas_call(
        functools.partial(kernel, (gz, gy, depth, cp)),
        out_shape=(
            jax.ShapeDtypeStruct(source.shape, f32),
            jax.ShapeDtypeStruct((8, 128), f32),
        ),
        in_specs=[vm, vm, pl.BlockSpec(memory_space=pltpu.SMEM), vm] + [vm] * len(consts),
        out_specs=(vm, vm),
        scratch_shapes=[
            pltpu.VMEM((2, depth + 2, n0, n0), f32),
            pltpu.VMEM((2, depth + 2, n1, n1), f32),
            pltpu.VMEM((depth, n0, n0), f32),
            pltpu.VMEM((depth, n1, n1), f32),
            pltpu.VMEM((depth, n1, n1), f32),
            pltpu.VMEM((depth, n1, n1), f32),
            pltpu.VMEM((depth, n1, n1), f32),
            pltpu.VMEM((n0, n1), f32),
            pltpu.VMEM((depth, n1, n1), f32),
            pltpu.VMEM((gz, cp), f32),
            pltpu.VMEM((gy, gz, depth, cp), f32),
            pltpu.VMEM((gy, gz, depth, cp), f32),
            pltpu.VMEM((gy, gz, depth, cp), f32),
            pltpu.VMEM((gy, gz, depth, cp), f32),
            pltpu.VMEM((2, gy, gz, depth, cp), f32),
            pltpu.VMEM((gy, gz, depth, cp), f32),
            pltpu.VMEM((gy, gz, 8, 128), f32),
            pltpu.VMEM((zall, cp), f32),
            pltpu.VMEM((nl, zall, cp), f32),
            pltpu.VMEM((nl, 2 * steps + 1, zall, cp), f32),
            pltpu.VMEM((nl, zall, cp), f32),
            pltpu.VMEM((2, zall, cp), f32),
            pltpu.VMEM((2, 4, zall, cp), f32),
            pltpu.VMEM((zall, cp), f32),
            pltpu.VMEM((CYCLES, 8, n0), f32),
            pltpu.SemaphoreType.DMA((2, 2, 2)),
            pltpu.SemaphoreType.DMA((2, 2, 2)),
            pltpu.SemaphoreType.DMA((2, 4)),
            pltpu.SemaphoreType.DMA((2, 4)),
            pltpu.SemaphoreType.DMA((5, nd)),
            pltpu.SemaphoreType.DMA((5, nd)),
        ],
        compiler_params=pltpu.CompilerParams(
            has_side_effects=True, vmem_limit_bytes=64000 * 1024
        ),
    )(
        source,
        reaction,
        vertical,
        jnp.broadcast_to(vertical[:, None], (depth, cp)),
        *[jnp.asarray(c) for c in consts],
    )
    return solution, norms[:CYCLES, 0]


def solution(mesh):
    return jax.shard_map(
        functools.partial(shards, mesh.shape["gz"], mesh.shape["gy"]),
        mesh=mesh,
        in_specs=(P(("gz", "gy"), None, None), P(("gz", "gy")), P(("gz", "gy"), None, None)),
        out_specs=(P(("gz", "gy"), None, None), P()),
        check_vma=False,
    )
```

```python
import functools

import jax
import jax.numpy as jnp
import numpy as np
from jax import lax
from jax.experimental import pallas as pl
from jax.experimental.pallas import tpu as pltpu
from jax.sharding import PartitionSpec as P

LEVELS = 5
SWITCH = 2
CYCLES = 2
SWEEPS = 2
COARSE = 4
DAMPING = 0.8
COUPLING = 1.0
CHUNK = 32
MESH = pl.DeviceIdType.MESH


def dot(a, b):
    return lax.dot_general(
        a,
        b,
        (((1,), (0,)), ((), ())),
        precision=lax.Precision.HIGHEST,
        preferred_element_type=jnp.float32,
    )


def parts_of(x):
    first = x.astype(jnp.bfloat16)
    rest = x - first.astype(jnp.float32)
    second = rest.astype(jnp.bfloat16)
    third = (rest - second.astype(jnp.float32)).astype(jnp.bfloat16)
    return (third, second, first)


def dot_right(x, m):
    m = m.astype(jnp.bfloat16)
    total = None
    for x in parts_of(x):
        term = jnp.dot(x, m, preferred_element_type=jnp.float32)
        total = term if total is None else total + term
    return total


def dot_left(m, x):
    m = m.astype(jnp.bfloat16)
    total = None
    for x in parts_of(x):
        term = jnp.dot(m, x, preferred_element_type=jnp.float32)
        total = term if total is None else total + term
    return total


def kernel(
    dims,
    source, reaction, vert_s, vert_b, down0, downt0, down1, cols, mask, group, ups, groupt, colst,
    out, norms,
    v0, v1, w0, d1, w1, g1, r1, tmp0, res1, corr1, send_a, recv_a, send_v, recv_v, recv_b,
    send_n, recv_n, lines, diag, factor, target, around, halo, rowbuf, acc,
    plane_send, plane_recv, line_send, line_recv, a2a_send, a2a_recv,
):
    gz, gy, depth, cp = dims
    nd = gz * gy
    zall = nd * depth
    n0 = source.shape[1]
    n1 = n0 // 2
    a_me = lax.axis_index("gz")
    b_me = lax.axis_index("gy")
    me = a_me * gy + b_me
    h = [COUPLING / 4.0**k for k in range(LEVELS)]

    @pl.when(me == 0)
    def _():
        for p in range(2):
            v0[p, 0] = jnp.zeros((n0, n0), jnp.float32)
            v1[p, 0] = jnp.zeros((n1, n1), jnp.float32)

    @pl.when(me == nd - 1)
    def _():
        for p in range(2):
            v0[p, depth + 1] = jnp.zeros((n0, n0), jnp.float32)
            v1[p, depth + 1] = jnp.zeros((n1, n1), jnp.float32)

    edges = [a_me == 0, a_me == gz - 1, b_me == 0, b_me == gy - 1]
    for k in range(4):
        @pl.when(edges[k])
        def _(k=k):
            for p in range(2):
                halo[p, k] = jnp.zeros((zall, cp), jnp.float32)

    def flat(d):
        return (d // gy, d % gy)

    def plane_copy(v, p, level, up):
        if up:
            src, dst, to = v.at[p, depth], v.at[p, 0], flat(me + 1)
        else:
            src, dst, to = v.at[p, 1], v.at[p, depth + 1], flat(me + nd - 1 - nd * ((me + nd - 1) // nd))
        if up:
            to = flat((me + 1) % nd)
        k = 0 if up else 1
        return pltpu.make_async_remote_copy(
            src_ref=src, dst_ref=dst,
            send_sem=plane_send.at[level, p, k], recv_sem=plane_recv.at[level, p, k],
            device_id=to, device_id_type=MESH,
        )

    def plane_start(v, p, level):
        @pl.when(me < nd - 1)
        def _():
            plane_copy(v, p, level, True).start()

        @pl.when(me > 0)
        def _():
            plane_copy(v, p, level, False).start()

    def plane_wait(v, p, level):
        @pl.when(me < nd - 1)
        def _():
            plane_copy(v, p, level, True).wait_send()
            plane_copy(v, p, level, False).wait_recv()

        @pl.when(me > 0)
        def _():
            plane_copy(v, p, level, False).wait_send()
            plane_copy(v, p, level, True).wait_recv()

    def residual_chunk(v, p, z, r, n, target_ref, diag_of, weight):
        centre = v[p, z, pl.ds(r, CHUNK), :]
        rows = lax.broadcasted_iota(jnp.int32, (CHUNK, n), 0)
        lanes = lax.broadcasted_iota(jnp.int32, (CHUNK, n), 1)
        if r == 0:
            above = jnp.where(rows == 0, 0.0, pltpu.roll(centre, 1, 0))
        else:
            above = v[p, z, pl.ds(r - 1, CHUNK), :]
        if r + CHUNK == n:
            below = jnp.where(rows == CHUNK - 1, 0.0, pltpu.roll(centre, CHUNK - 1, 0))
        else:
            below = v[p, z, pl.ds(r + 1, CHUNK), :]
        left = jnp.where(lanes == 0, 0.0, pltpu.roll(centre, 1, 1))
        right = jnp.where(lanes == n - 1, 0.0, pltpu.roll(centre, n - 1, 1))
        vert = vert_s[z - 1]
        applied = (
            diag_of(z - 1, r, vert) * centre
            - vert * (v[p, z - 1, pl.ds(r, CHUNK), :] + v[p, z + 1, pl.ds(r, CHUNK), :])
            - weight * (above + below + left + right)
        )
        return centre, target_ref[z - 1, pl.ds(r, CHUNK), :] - applied

    def diag0(z, r, vert):
        return 2.0 * vert + 4.0 * h[0] + reaction[z, pl.ds(r, CHUNK), :]

    def diag1(z, r, vert):
        return d1[z, pl.ds(r, CHUNK), :]

    def over_planes(v, p, level, body):
        plane_start(v, p, level)

        def inner(z, c):
            body(z)
            return c

        lax.fori_loop(2, depth, inner, 0)
        plane_wait(v, p, level)

        def outer(i, c):
            body(1 + i * (depth - 1))
            return c

        lax.fori_loop(0, 2, outer, 0)

    def level_parts(level):
        if level == 0:
            return v0, source, diag0, w0, n0
        return v1, g1, diag1, w1, n1

    def sweep(level, p, record=None):
        v, tgt, dg, w, n = level_parts(level)

        def body(z):
            for r in range(0, n, CHUNK):
                centre, res = residual_chunk(v, p, z, r, n, tgt, dg, h[level])
                v[1 - p, z, pl.ds(r, CHUNK), :] = centre + w[z - 1, pl.ds(r, CHUNK), :] * res
                if record is not None:
                    sq = (res * res).reshape(CHUNK // 8, 8, n).sum(axis=0)
                    acc[record, :, :] += sq

        over_planes(v, p, level, body)
        return 1 - p

    def first_sweep(level):
        v, tgt, dg, w, n = level_parts(level)

        def body(z, c):
            v[0, z + 1] = w[z] * tgt[z]
            return c

        lax.fori_loop(0, depth, body, 0)
        return 0

    def restrict0(read_chunk, store):
        def body(z):
            for r in range(0, n0, CHUNK):
                tmp0[pl.ds(r, CHUNK), :] = dot_right(read_chunk(z, r), downt0[...])
            store(z, dot_left(down0[...], tmp0[...]))
        return body

    def restrict1(z, plane):
        half = dot(down1[...], plane)
        for b in range(gy):
            spread = dot(half, cols[b]) * mask[...]
            packed = dot(group[...], spread)
            for a in range(gz):
                send_a[b, a, z : z + 1, :] = packed[a : a + 1, :]

    def exchange_all(kind, src_of, recv):
        def copy(k):
            dst = (me + k) % nd
            a, b = dst // gy, dst % gy
            return pltpu.make_async_remote_copy(
                src_ref=src_of(a, b), dst_ref=recv.at[b_me, a_me],
                send_sem=a2a_send.at[kind, k], recv_sem=a2a_recv.at[kind, me],
                device_id=(a, b), device_id_type=MESH,
            )

        def start(k, c):
            copy(k).start()
            return c

        def finish(k, c):
            copy(k).wait_send()
            src = (me + k) % nd
            a, b = src // gy, src % gy
            pltpu.make_async_remote_copy(
                src_ref=recv.at[b, a], dst_ref=recv.at[b, a],
                send_sem=a2a_send.at[kind, k], recv_sem=a2a_recv.at[kind, src],
                device_id=(a, b), device_id_type=MESH,
            ).wait_recv()
            return c

        def begin():
            lax.fori_loop(1, nd, start, 0)

        def end():
            lax.fori_loop(1, nd, finish, 0)

        return begin, end

    def to_lines(recv, dest):
        for a in range(gz):
            for b in range(gy):
                s = (a * gy + b) * depth
                dest[s : s + depth, :] = recv[b, a]

    bx2, by2 = (n1 // 2 // gz, n1 // 2 // gy)
    steps = []
    s = 1
    while s < zall:
        steps.append(s)
        s *= 2
    ns = len(steps)

    def setup_lines(offset):
        rows = lax.broadcasted_iota(jnp.int32, (zall, cp), 0)
        vert = lines[...]
        a = jnp.where(rows == 0, 0.0, -vert)
        c = jnp.where(rows == zall - 1, 0.0, -vert)
        b = diag[offset]
        for k, s in enumerate(steps):
            alpha = -a / pltpu.roll(b, s, 0)
            gamma = -c / pltpu.roll(b, zall - s, 0)
            b = b + alpha * pltpu.roll(c, s, 0) + gamma * pltpu.roll(a, zall - s, 0)
            a = alpha * pltpu.roll(a, s, 0)
            c = gamma * pltpu.roll(c, zall - s, 0)
            factor[offset, 2 * k] = alpha
            factor[offset, 2 * k + 1] = gamma
        factor[offset, 2 * ns] = 1.0 / b

    def solve(offset, right):
        for k, s in enumerate(steps):
            right = (
                right
                + factor[offset, 2 * k] * pltpu.roll(right, s, 0)
                + factor[offset, 2 * k + 1] * pltpu.roll(right, zall - s, 0)
            )
        return right * factor[offset, 2 * ns]

    count = [0]
    def line_copy(p, k):
        if k == 0:
            to, slot = ((a_me + gz - 1) % gz, b_me), 1
        elif k == 1:
            to, slot = ((a_me + 1) % gz, b_me), 0
        elif k == 2:
            to, slot = (a_me, (b_me + gy - 1) % gy), 3
        else:
            to, slot = (a_me, (b_me + 1) % gy), 2
        return pltpu.make_async_remote_copy(
            src_ref=around.at[p], dst_ref=halo.at[p, slot],
            send_sem=line_send.at[p, k], recv_sem=line_recv.at[p, slot],
            device_id=to, device_id_type=MESH,
        )

    def line_landed(p, k):
        return pltpu.make_async_remote_copy(
            src_ref=around.at[p], dst_ref=halo.at[p, k],
            send_sem=line_send.at[p, k], recv_sem=line_recv.at[p, k],
            device_id=(a_me, b_me), device_id_type=MESH,
        )

    def neighbours(offset, values):
        bx, by = bx2 >> offset, by2 >> offset
        cells = bx * by
        p = count[0] % 2
        count[0] += 1
        around[p] = values
        for k in range(4):
            @pl.when(jnp.logical_not(edges[k]))
            def _(k=k):
                line_copy(p, k).start()
        for k in range(4):
            @pl.when(jnp.logical_not(edges[k]))
            def _(k=k):
                line_copy(p, k).wait_send()
                line_landed(p, k).wait_recv()
        lane = lax.broadcasted_iota(jnp.int32, (zall, cp), 1)

        def roll(x, amount):
            amount = amount % cp
            return x if amount == 0 else pltpu.roll(x, amount, 1)

        total = jnp.where(lane < by, roll(halo[p, 0], by - cells), roll(values, by))
        total += jnp.where(lane >= cells - by, roll(halo[p, 1], cells - by), roll(values, -by))
        inrow = lane & (by - 1)
        total += jnp.where(inrow == 0, roll(halo[p, 2], 1 - by), roll(values, 1))
        total += jnp.where(inrow == by - 1, roll(halo[p, 3], by - 1), roll(values, -1))
        return total

    def line_descend(offset):
        weight = h[SWITCH + offset]
        values = solve(offset, target[offset])
        repeats = COARSE if offset == LEVELS - 1 - SWITCH else SWEEPS
        for _ in range(1, repeats):
            values = solve(offset, target[offset] + weight * neighbours(offset, values))
        if offset == LEVELS - 1 - SWITCH:
            return values
        near = neighbours(offset, values)
        rows = lax.broadcasted_iota(jnp.int32, (zall, cp), 0)
        before = jnp.where(rows == 0, 0.0, pltpu.roll(values, 1, 0))
        after = jnp.where(rows == zall - 1, 0.0, pltpu.roll(values, zall - 1, 0))
        res = target[offset] - (
            diag[offset] * values - lines[...] * (before + after) - weight * near
        )
        target[offset + 1] = dot(res, ups[2 * offset])
        tmp = values
        lower = line_descend(offset + 1)
        values = tmp + dot(lower, ups[2 * offset + 1])
        for _ in range(SWEEPS):
            values = solve(offset, target[offset] + weight * neighbours(offset, values))
        return values

    def fill0(z, c):
        w0[z] = DAMPING / (2.0 * vert_s[z] + 4.0 * h[0] + reaction[z])
        return c

    lax.fori_loop(0, depth, fill0, 0)

    def keep_r1(z, value):
        r1[z] = value
        dv = 2.0 * vert_s[z] + 4.0 * h[1] + value
        d1[z] = dv
        w1[z] = DAMPING / dv

    body = restrict0(lambda z, r: reaction[z, pl.ds(r, CHUNK), :], keep_r1)
    lax.fori_loop(0, depth, lambda z, c: (body(z), c)[1], 0)
    for z in range(depth):
        restrict1(z, r1[z])
    send_v[...] = send_a[...]
    begin_v, end_v = exchange_all(0, lambda a, b: vert_b, recv_v)
    begin_r, end_r = exchange_all(1, lambda a, b: send_v.at[b, a], recv_a)
    begin_v()
    begin_r()
    recv_v[b_me, a_me] = vert_b[...]
    recv_a[b_me, a_me] = send_v[b_me, a_me]
    acc[...] = jnp.zeros_like(acc)

    begin_a, end_a = exchange_all(2, lambda a, b: send_a.at[b, a], recv_b.at[0])
    begin_b, end_b = exchange_all(3, lambda a, b: send_n.at[b, a], recv_b.at[1])

    p0 = first_sweep(0)
    for cycle in range(CYCLES):
        for k in range(SWEEPS):
            if cycle == 0 and k == 0:
                continue
            p0 = sweep(0, p0, record=cycle - 1 if cycle > 0 and k == 0 else None)

        def read0(z, r, p0=p0):
            return residual_chunk(v0, p0, z, r, n0, source, diag0, h[0])[1]

        def keep_g1(z, value):
            g1[z - 1] = value

        over_planes(v0, p0, 0, restrict0(read0, keep_g1))
        p1 = first_sweep(1)
        for k in range(1, SWEEPS):
            p1 = sweep(1, p1)

        def keep_res(z, p1=p1):
            for r in range(0, n1, CHUNK):
                res1[z - 1, pl.ds(r, CHUNK), :] = residual_chunk(
                    v1, p1, z, r, n1, g1, diag1, h[1]
                )[1]

        over_planes(v1, p1, 1, keep_res)
        for z in range(depth):
            restrict1(z, res1[z])
        begin_a()
        recv_b[0, b_me, a_me] = send_a[b_me, a_me]
        if cycle == 0:
            end_v()
            end_r()
            to_lines(recv_v, lines)
            to_lines(recv_a, target.at[0])
            coarse = target[0]
            for offset in range(LEVELS - SWITCH):
                if offset > 0:
                    coarse = dot(coarse, ups[2 * offset - 2])
                diag[offset] = 2.0 * lines[...] + 4.0 * h[SWITCH + offset] + coarse
            for offset in range(LEVELS - SWITCH):
                setup_lines(offset)
        end_a()
        to_lines(recv_b.at[0], target.at[0])
        rowbuf[...] = line_descend(0)
        for a in range(gz):
            for b in range(gy):
                s = (a * gy + b) * depth
                send_n[b, a] = rowbuf[s : s + depth, :]
        begin_b()
        recv_b[1, b_me, a_me] = send_n[b_me, a_me]
        end_b()
        for z in range(depth):
            wide = None
            for b in range(gy):
                for a in range(gz):
                    corr1[a : a + 1, :] = recv_b[1, b, a, z : z + 1, :]
                part = dot(dot(groupt[...], corr1[...]) * mask[...], colst[b])
                wide = part if wide is None else wide + part
            v1[1 - p1, z + 1] = v1[p1, z + 1] + dot(down1[...].T * 2.0, wide)
        p1 = 1 - p1
        for _ in range(SWEEPS):
            p1 = sweep(1, p1)

        def correct0(z, c, p0=p0, p1=p1):
            tmp0[...] = dot_left(downt0[...] * 2.0, v1[p1, z])
            for r in range(0, n0, CHUNK):
                v0[1 - p0, z, pl.ds(r, CHUNK), :] = v0[p0, z, pl.ds(r, CHUNK), :] + dot_right(
                    tmp0[pl.ds(r, CHUNK), :], down0[...] * 2.0
                )
            return c

        lax.fori_loop(1, depth + 1, correct0, 0)
        p0 = 1 - p0
        for _ in range(SWEEPS):
            p0 = sweep(0, p0)

    def last(z, p0=p0):
        for r in range(0, n0, CHUNK):
            centre, res = residual_chunk(v0, p0, z, r, n0, source, diag0, h[0])
            out[z - 1, pl.ds(r, CHUNK), :] = centre
            acc[CYCLES - 1, :, :] += (res * res).reshape(CHUNK // 8, 8, n0).sum(axis=0)

    over_planes(v0, p0, 0, last)
    ridx = lax.broadcasted_iota(jnp.int32, (8, 128), 0)
    part = jnp.zeros((8, 128), jnp.float32)
    for k in range(CYCLES):
        part = jnp.where(ridx == k, jnp.sum(acc[k]), part)
    rowbuf_n = tmp_n = send_n
    target_n = recv_n
    w_n = acc
    acc[0, :, 0:128] = part
    begin_n, end_n = exchange_all(4, lambda a, b: acc.at[0, :, pl.ds(0, 128)], recv_n)
    begin_n()
    recv_n[b_me, a_me] = part
    end_n()
    total = jnp.zeros((8, 128), jnp.float32)
    for a in range(gz):
        for b in range(gy):
            total = total + recv_n[b, a]
    norms[...] = total * (1.0 / (zall * n0 * n0))


def pair_matrix(n, value):
    return (np.arange(n)[None, :] // 2 == np.arange(n // 2)[:, None]).astype(np.float32) * value


def shards(gz, gy, source, vertical, reaction):
    depth, n0 = source.shape[0], source.shape[1]
    nd = gz * gy
    zall = nd * depth
    n1, n2 = n0 // 2, n0 // 4
    bx, by = n2 // gz, n2 // gy
    cells = bx * by
    cp = -(-cells // 128) * 128
    down0 = pair_matrix(n0, 0.5)
    down1 = pair_matrix(n1, 0.5)
    lane = np.arange(cp)
    cols = np.zeros((gy, n1, cp), np.float32)
    colst = np.zeros((gy, cp, n1), np.float32)
    for b in range(gy):
        hit = (np.arange(n1)[:, None] // 2 == b * by + lane[None, :] % by) & (lane[None, :] < cells)
        cols[b] = hit * 0.5
        colst[b] = hit.T
    mask = ((lane[None, :] // by == np.arange(n2)[:, None] % bx) & (lane[None, :] < cells)).astype(np.float32)
    group = (np.arange(n2)[None, :] // bx == np.arange(gz)[:, None]).astype(np.float32)
    ups = []
    for offset in range(LEVELS - SWITCH - 1):
        fx, fy = bx >> offset, by >> offset
        cy = fy // 2
        matrix = np.zeros((cp, cp), np.float32)
        for i in range(fx):
            for j in range(fy):
                matrix[i * fy + j, (i // 2) * cy + j // 2] = 1.0
        ups += [matrix * 0.25, matrix.T]
    ups = np.stack(ups)
    steps = (zall - 1).bit_length()
    f32 = jnp.float32
    nl = LEVELS - SWITCH
    vm = pl.BlockSpec(memory_space=pltpu.VMEM)
    consts = [down0, down0.T.copy(), down1, cols, mask, group, ups, group.T.copy(), colst]
    solution, norms = pl.pallas_call(
        functools.partial(kernel, (gz, gy, depth, cp)),
        out_shape=(
            jax.ShapeDtypeStruct(source.shape, f32),
            jax.ShapeDtypeStruct((8, 128), f32),
        ),
        in_specs=[vm, vm, pl.BlockSpec(memory_space=pltpu.SMEM), vm] + [vm] * len(consts),
        out_specs=(vm, vm),
        scratch_shapes=[
            pltpu.VMEM((2, depth + 2, n0, n0), f32),
            pltpu.VMEM((2, depth + 2, n1, n1), f32),
            pltpu.VMEM((depth, n0, n0), f32),
            pltpu.VMEM((depth, n1, n1), f32),
            pltpu.VMEM((depth, n1, n1), f32),
            pltpu.VMEM((depth, n1, n1), f32),
            pltpu.VMEM((depth, n1, n1), f32),
            pltpu.VMEM((n0, n1), f32),
            pltpu.VMEM((depth, n1, n1), f32),
            pltpu.VMEM((gz, cp), f32),
            pltpu.VMEM((gy, gz, depth, cp), f32),
            pltpu.VMEM((gy, gz, depth, cp), f32),
            pltpu.VMEM((gy, gz, depth, cp), f32),
            pltpu.VMEM((gy, gz, depth, cp), f32),
            pltpu.VMEM((2, gy, gz, depth, cp), f32),
            pltpu.VMEM((gy, gz, depth, cp), f32),
            pltpu.VMEM((gy, gz, 8, 128), f32),
            pltpu.VMEM((zall, cp), f32),
            pltpu.VMEM((nl, zall, cp), f32),
            pltpu.VMEM((nl, 2 * steps + 1, zall, cp), f32),
            pltpu.VMEM((nl, zall, cp), f32),
            pltpu.VMEM((2, zall, cp), f32),
            pltpu.VMEM((2, 4, zall, cp), f32),
            pltpu.VMEM((zall, cp), f32),
            pltpu.VMEM((CYCLES, 8, n0), f32),
            pltpu.SemaphoreType.DMA((2, 2, 2)),
            pltpu.SemaphoreType.DMA((2, 2, 2)),
            pltpu.SemaphoreType.DMA((2, 4)),
            pltpu.SemaphoreType.DMA((2, 4)),
            pltpu.SemaphoreType.DMA((5, nd)),
            pltpu.SemaphoreType.DMA((5, nd)),
        ],
        compiler_params=pltpu.CompilerParams(
            has_side_effects=True, vmem_limit_bytes=64000 * 1024
        ),
    )(
        source,
        reaction,
        vertical,
        jnp.broadcast_to(vertical[:, None], (depth, cp)),
        *[jnp.asarray(c) for c in consts],
    )
    return solution, norms[:CYCLES, 0]


def solution(mesh):
    return jax.shard_map(
        functools.partial(shards, mesh.shape["gz"], mesh.shape["gy"]),
        mesh=mesh,
        in_specs=(P(("gz", "gy"), None, None), P(("gz", "gy")), P(("gz", "gy"), None, None)),
        out_specs=(P(("gz", "gy"), None, None), P()),
        check_vma=False,
    )
```
